32 devices in a mesh: rows: 4 (over z), cols: 4 (over y, x), space: 2 (over core).
Axes of the slice: x: 2, y: 2, z: 4, core: 2. Of those that a mesh axis runs over, the one named last changes fastest.
Arguments:
- hamiltonian: float32 [2048, 1536], P(('rows', 'cols', 'space')), may hold values from -1 to 1
- correlation_root: float32 [2048, 1536], P('rows'), may hold values from -1 to 2
- pattern: int32 [64, 48], replicated, may hold values from 0 to 1
- sub_blocks: int32 [64, 16], P(('rows', 'cols', 'space')), may hold values from 0 to 47, as said below
- sub_count: int32 [64], P(('rows', 'cols', 'space')), may hold values from 8 to 16, as said below
Outputs:
- density: float32 [2048, 1536], P(('rows', 'cols', 'space'))
- charges: float32 [2048], P(('rows', 'cols', 'space'))
The draws below stay inside these ranges and needn't reach their ends.
Inputs may be any that keep to these rules, and one draw needn't show every extreme that they name: `sub_blocks`: row g lists distinct positions; its first entry is 16 + g mod 16, the position of block g itself. `sub_count`: some submatrix has exactly 16 live blocks.
All inputs are finite; a program needn't handle non-finite values.
Results may differ from the reference program's by a relative error of at most 0.0003.
Values sent between devices are 32-bit elements; how exact they have to be, the bound alone decides.
A program may use at most 128 MiB of HBM per device.

```python
import math
import jax
import jax.numpy as jnp
from jax import lax

BLK = 32
MAXB = 16
NPG = 16
SLAB = 512
WIN = 1536
WB = 48
NB = 64
N = 2048
N_ROWS = 4


def draw_hamiltonian(key, part):
    values = jnp.clip(jax.random.normal(key, (N, WIN), jnp.float32), -6.0, 6.0)
    return values / math.sqrt(WIN)


def draw_correlation_root(key, part):
    entries = jnp.clip(jax.random.normal(key, (N, WIN), jnp.float32), -6.0, 6.0)
    entries = entries * (0.6 / math.sqrt(WIN))
    row_ids = jnp.arange(N, dtype=jnp.int32)
    column_ids = jnp.arange(WIN, dtype=jnp.int32)
    diagonal = (column_ids[None, :] == SLAB + (row_ids % SLAB)[:, None]).astype(jnp.float32)
    return entries + diagonal


def draw_pattern(key, part):
    picks = jax.random.randint(key, (NB, WB), 0, 5)
    block_ids = jnp.arange(NB, dtype=jnp.int32)
    band_ids = jnp.arange(WB, dtype=jnp.int32)
    diagonal = band_ids[None, :] == NPG + (block_ids % NPG)[:, None]
    return jnp.where(diagonal | (picks < 3), 1, 0).astype(jnp.int32)


def draw_sub_blocks(key, part):
    key_list = jax.random.split(jax.random.fold_in(key, 11), NB)
    shuffled = jax.vmap(lambda single: jax.random.permutation(single, WB - 1))(key_list).astype(jnp.int32)
    home_slot = (NPG + jnp.arange(NB, dtype=jnp.int32) % NPG)[:, None]
    neighbours = shuffled + (shuffled >= home_slot).astype(jnp.int32)
    return jnp.concatenate([home_slot, neighbours[:, :MAXB - 1]], axis=1).astype(jnp.int32)


def draw_sub_count(key, part):
    block_counts = jax.random.randint(jax.random.fold_in(key, 5), (NB,), MAXB // 2, MAXB + 1)
    chosen_block = jax.random.randint(jax.random.fold_in(key, 6), (), 0, NB)
    return jnp.where(jnp.arange(NB, dtype=jnp.int32) == chosen_block, MAXB, block_counts).astype(jnp.int32)


def setup_inputs(seed: int = 0) -> dict:
    arg_keys = jax.random.split(jax.random.key(seed), 6)
    hamiltonian = draw_hamiltonian(jax.random.fold_in(arg_keys[5], 71), 0)
    correlation_root = draw_correlation_root(jax.random.fold_in(arg_keys[5], 71), 0)
    pattern = draw_pattern(jax.random.fold_in(arg_keys[5], 71), 0)
    sub_blocks = draw_sub_blocks(jax.random.fold_in(arg_keys[5], 71), 0)
    sub_count = draw_sub_count(jax.random.fold_in(arg_keys[5], 71), 0)
    return dict(hamiltonian=hamiltonian, correlation_root=correlation_root, pattern=pattern, sub_blocks=sub_blocks, sub_count=sub_count)


highest = lax.Precision.HIGHEST

def multiply(leftside, rightside):
    return jnp.dot(leftside, rightside, precision=highest, preferred_element_type=jnp.float32)

def windows(banded):
    stacked = banded.reshape(N_ROWS, SLAB, WIN)
    above_used = jnp.roll(stacked, 1, axis=0)[:, :, SLAB:]
    below_used = jnp.roll(stacked, -1, axis=0)[:, :, :2 * SLAB]
    zero_block = jnp.zeros((N_ROWS, SLAB, SLAB), jnp.float32)
    top_rows = jnp.concatenate([above_used, zero_block], axis=2)
    bottom = jnp.concatenate([zero_block, below_used], axis=2)
    return jnp.concatenate([top_rows, stacked, bottom], axis=1)

def sandwich_step(leftside, rightside, pattern_mask):
    stacked = leftside.reshape(N_ROWS, SLAB, WIN)
    joined = jnp.einsum('sik,skj->sij', stacked, windows(rightside), precision=highest)
    return pattern_mask * joined.reshape(N, WIN)

def density_rows(local_window, positions, live_count):
    offsets = (positions[:, None] * BLK + jnp.arange(BLK, dtype=jnp.int32)[None, :]).reshape(-1)
    live_cols = jnp.repeat((jnp.arange(MAXB, dtype=jnp.int32) < live_count).astype(jnp.float32), BLK)
    assembled = jnp.take(jnp.take(local_window, offsets, axis=0), offsets, axis=1)
    assembled = assembled * live_cols[:, None] * live_cols[None, :]
    symmetric = 0.5 * (assembled + assembled.T)
    live_order = (live_count * BLK).astype(jnp.float32)
    normalizer = jnp.sqrt(live_order) / (2.0 * jnp.sqrt(jnp.sum(symmetric * symmetric) + 1e-06))
    iterate = symmetric * normalizer
    square = multiply(iterate, iterate)
    iterate = 1.5 * iterate - 0.5 * multiply(iterate, square)
    square = multiply(iterate, iterate)
    home_rows = iterate[:BLK]
    home_rows = 1.5 * home_rows - 0.5 * multiply(home_rows, square)
    padded_order = MAXB * BLK
    home_eye = (jnp.arange(BLK, dtype=jnp.int32)[:, None] == jnp.arange(padded_order, dtype=jnp.int32)[None, :]).astype(jnp.float32)
    home_density = 0.5 * (home_eye - home_rows)
    placement = (offsets[:, None] == jnp.arange(local_window.shape[1], dtype=jnp.int32)[None, :]).astype(jnp.float32)
    return multiply(home_density, placement)

def reference(hamiltonian, correlation_root, pattern, sub_blocks, sub_count):
    pattern_mask = jnp.repeat(jnp.repeat(pattern.astype(jnp.float32), BLK, axis=0), BLK, axis=1)
    half_done = sandwich_step(hamiltonian, correlation_root, pattern_mask)
    orthogonal = sandwich_step(correlation_root, half_done, pattern_mask)
    ortho_windows = windows(orthogonal)

    def solve_block(entries):
        block_index, positions, live_count = entries
        slab_index = (block_index // NPG).astype(jnp.int32)
        local_window = lax.dynamic_index_in_dim(ortho_windows, slab_index, 0, keepdims=False)
        return density_rows(local_window, positions, live_count)
    density_blocks = lax.map(solve_block, (jnp.arange(NB, dtype=jnp.int32), sub_blocks, sub_count))
    density_band = density_blocks.reshape(N, WIN)
    half_back = sandwich_step(density_band, correlation_root, pattern_mask)
    density = sandwich_step(correlation_root, half_back, pattern_mask)
    charges = lax.optimization_barrier(jnp.sum(density, axis=1))
    return (density, charges)
```

```python
import functools

import jax
import jax.numpy as jnp
from jax import lax
from jax.experimental import pallas as pl
from jax.experimental.pallas import tpu as pltpu
from jax.sharding import PartitionSpec as P

BLK = 32
GROUP = ("cols", "space")


def passed_along(value, axis, steps):
    count = lax.axis_size(axis)
    pairs = [(source, (source + steps) % count) for source in range(count)]
    return lax.ppermute(value, axis, pairs)


def multiply_nt(leftside, rightside):
    return lax.dot_general(
        leftside,
        rightside,
        (((1,), (1,)), ((), ())),
        precision=lax.Precision.HIGH,
        preferred_element_type=jnp.float32,
    )


def neighbour_panels(piece):
    above = passed_along(piece[1:], "rows", 1)
    below = passed_along(piece[:2], "rows", -1)
    return above, below


def window_columns(piece, above, below):
    zero = jnp.zeros(piece.shape[1:], piece.dtype)
    rows = [
        jnp.concatenate([above[0], piece[0], zero], axis=1),
        jnp.concatenate([above[1], piece[1], below[0]], axis=1),
        jnp.concatenate([zero, piece[2], below[1]], axis=1),
    ]
    return jnp.concatenate(rows, axis=0)


def split(value):
    upper = value.astype(jnp.bfloat16)
    return upper, (value - upper.astype(jnp.float32)).astype(jnp.bfloat16)


def dot_f32(leftside, rightside):
    return jnp.dot(leftside, rightside, preferred_element_type=jnp.float32)


def dot_split(leftside, rightside):
    left_hi, left_lo = leftside
    right_hi, right_lo = rightside
    return (
        dot_f32(left_hi, right_hi)
        + dot_f32(left_hi, right_lo)
        + dot_f32(left_lo, right_hi)
    )


def submatrix_kernel(maxb, slab_blocks, pos_ref, count_ref, offs_ref, gathered_ref, out_ref, rows_ref):
    width = gathered_ref.shape[2]
    slab = gathered_ref.shape[3]
    per_piece = width // BLK
    index = pl.program_id(0)
    live = count_ref[index]

    def place(p, carry):
        block = pos_ref[index, p]
        panel = block // slab_blocks
        within = lax.rem(block, slab_blocks)
        owner = within // per_piece
        start = pl.multiple_of(lax.rem(within, per_piece) * BLK, BLK)
        target = pl.multiple_of(p * BLK, BLK)
        for a in range(3):
            keep = (jnp.abs(panel - a) <= 1) & (p < live)
            values = gathered_ref[owner, 2 * panel + a, pl.ds(start, BLK), :]
            rows_ref[pl.ds(target, BLK), a * slab : (a + 1) * slab] = jnp.where(keep, values, 0.0)
        return carry

    lax.fori_loop(0, maxb, place, 0)
    offsets = offs_ref[0]
    order = maxb * BLK
    select = lax.broadcasted_iota(jnp.int32, (3 * slab, order), 0) == offsets
    select = jnp.where(select, 1.0, 0.0).astype(jnp.bfloat16)
    rows_hi, rows_lo = split(rows_ref[...])
    assembled = dot_f32(rows_hi, select) + dot_f32(rows_lo, select)
    columns = lax.broadcasted_iota(jnp.int32, (order, order), 1)
    assembled = jnp.where(columns < live * BLK, assembled, 0.0)
    symmetric = 0.5 * (assembled + assembled.T)
    total = jnp.sum(jnp.sum(symmetric * symmetric, axis=1, keepdims=True), axis=0, keepdims=True)
    live_order = jnp.full((1, 1), live * BLK, jnp.int32).astype(jnp.float32)
    iterate = symmetric * (jnp.sqrt(live_order) / (2.0 * jnp.sqrt(total + 1e-06)))
    parts = split(iterate)
    square = split(dot_split(parts, parts))
    iterate = 1.5 * iterate - 0.5 * dot_split(parts, square)
    home = iterate[:BLK]
    parts = split(iterate)
    once = dot_split((parts[0][:BLK], parts[1][:BLK]), parts)
    home = 1.5 * home - 0.5 * dot_split(split(once), parts)
    row = lax.broadcasted_iota(jnp.int32, (BLK, order), 0)
    column = lax.broadcasted_iota(jnp.int32, (BLK, order), 1)
    density = 0.5 * (jnp.where(row == column, 1.0, 0.0) - home)
    density_hi, density_lo = split(density)
    spread = functools.partial(
        lax.dot_general,
        dimension_numbers=(((1,), (1,)), ((), ())),
        preferred_element_type=jnp.float32,
    )
    out_ref[...] = spread(density_hi, select) + spread(density_lo, select)


def submatrices(gathered, sub_blocks, sub_count):
    own_blocks, maxb = sub_blocks.shape
    slab = gathered.shape[3]
    order = maxb * BLK
    offsets = sub_blocks[:, :, None] * BLK + jnp.arange(BLK, dtype=jnp.int32)
    offsets = offsets.reshape(own_blocks, 1, order)
    return pl.pallas_call(
        functools.partial(submatrix_kernel, maxb, slab // BLK),
        out_shape=jax.ShapeDtypeStruct((own_blocks * BLK, 3 * slab), jnp.float32),
        grid_spec=pltpu.PrefetchScalarGridSpec(
            num_scalar_prefetch=2,
            grid=(own_blocks,),
            in_specs=[
                pl.BlockSpec((1, 1, order), lambda i, *_: (i, 0, 0)),
                pl.BlockSpec(memory_space=pltpu.VMEM),
            ],
            out_specs=pl.BlockSpec((BLK, 3 * slab), lambda i, *_: (i, 0)),
            scratch_shapes=[pltpu.VMEM((order, 3 * slab), jnp.float32)],
        ),
    )(sub_blocks, sub_count, offsets, gathered)


def shards(hamiltonian, correlation_root, pattern, sub_blocks, sub_count):
    slab = correlation_root.shape[0]
    slab_blocks = slab // BLK
    own = hamiltonian.shape[0]
    parts = slab // own
    slab_index = lax.axis_index("rows")
    home = lax.axis_index(GROUP)
    slab_pattern = lax.dynamic_slice_in_dim(pattern, slab_index * slab_blocks, slab_blocks, 0)
    weights = slab_pattern.astype(jnp.float32)
    own_pattern = lax.dynamic_slice_in_dim(weights, home * (own // BLK), own // BLK, 0)
    own_mask = jnp.repeat(jnp.repeat(own_pattern, BLK, axis=0), BLK, axis=1)
    piece_pattern = lax.dynamic_index_in_dim(
        weights.reshape(slab_blocks, 3, parts, own // BLK), home, 2, keepdims=False
    )
    piece_mask = jnp.repeat(jnp.repeat(piece_pattern.transpose(1, 2, 0), BLK, axis=1), BLK, axis=2)

    whole_hamiltonian = lax.all_gather(hamiltonian, GROUP, axis=0, tiled=True)
    root_piece = lax.dynamic_index_in_dim(
        correlation_root.reshape(slab, 3, parts, own), home, 2, keepdims=False
    ).transpose(1, 2, 0)
    root_window = window_columns(root_piece, *neighbour_panels(root_piece))

    def step(left, window):
        return piece_mask * multiply_nt(window, left).reshape(piece_mask.shape)

    half_done = step(whole_hamiltonian, root_window)
    done_window = window_columns(half_done, *neighbour_panels(half_done))
    ortho = step(correlation_root, done_window)
    above, below = neighbour_panels(ortho)
    panels = jnp.stack([above[0], ortho[0], above[1], ortho[1], below[0], ortho[2], below[1]])
    gathered = lax.all_gather(panels, GROUP, axis=0, tiled=False)
    home_density = submatrices(gathered, sub_blocks, sub_count)
    whole_density = lax.all_gather(home_density, GROUP, axis=0, tiled=True)
    half_back = step(whole_density, root_window)
    back_window = window_columns(half_back, *neighbour_panels(half_back))
    density = multiply_nt(back_window, correlation_root).reshape(3, own, parts, own)
    density = lax.all_to_all(density.transpose(2, 3, 0, 1), GROUP, 0, 0, tiled=False)
    density = own_mask * density.transpose(1, 2, 0, 3).reshape(own, 3 * slab)
    return density, jnp.sum(density, axis=1)


def solution(mesh):
    return jax.shard_map(
        shards,
        mesh=mesh,
        in_specs=(
            P(("rows", "cols", "space"), None),
            P("rows", None),
            P(),
            P(("rows", "cols", "space"), None),
            P(("rows", "cols", "space")),
        ),
        out_specs=(P(("rows", "cols", "space"), None), P(("rows", "cols", "space"))),
        check_vma=False,
    )
```

```python
import functools

import jax
import jax.numpy as jnp
from jax import lax
from jax.experimental import pallas as pl
from jax.experimental.pallas import tpu as pltpu
from jax.sharding import PartitionSpec as P

BLK = 32
GROUP = ("cols", "space")


def multiply_nt(leftside, rightside):
    return lax.dot_general(
        leftside,
        rightside,
        (((1,), (1,)), ((), ())),
        precision=lax.Precision.HIGH,
        preferred_element_type=jnp.float32,
    )


class Sender:
    def __init__(self, send_sems, recv_sems):
        self.sems = (send_sems, recv_sems)
        self.copies = []

    def start(self, source, target, device):
        slot = len(self.copies)
        copy = pltpu.make_async_remote_copy(
            src_ref=source,
            dst_ref=target,
            send_sem=self.sems[0].at[slot],
            recv_sem=self.sems[1].at[slot],
            device_id=device,
            device_id_type=pl.DeviceIdType.MESH,
        )
        copy.start()
        self.copies.append(copy)
        return copy

    def finish(self):
        for copy in self.copies:
            copy.wait_send()


class Gather:
    def __init__(self, sender, source, out_ref, rows, lanes):
        self.sender, self.out_ref, self.rows, self.lanes = sender, out_ref, rows, lanes
        col = lax.axis_index("cols")
        space = lax.axis_index("space")
        self.first = col + 1 - 2 * lax.rem(col, 2)
        self.second = lax.rem(col + 2, 4)
        self.third = lax.rem(self.first + 2, 4)
        self.space = space
        own = self.region(col)
        self.from_first = sender.start(source, own, {"cols": self.first})
        self.from_second = sender.start(source, own, {"cols": self.second})
        self.pending = [sender.start(source, own, {"space": 1 - space})]

    def region(self, col, half=None):
        start, size = self.rows
        if half is not None:
            size = size // 2
            start = start + half * size
        owner = col * 2 + self.space
        return self.out_ref.at[owner, pl.ds(start, size), pl.ds(*self.lanes)]

    def partner(self, region):
        self.pending.append(self.sender.start(region, region, {"space": 1 - self.space}))

    def relay(self):
        self.from_first.wait_recv()
        passed = self.region(self.first, 1)
        self.half_second = self.sender.start(passed, passed, {"cols": self.second})
        self.partner(self.region(self.first))
        self.from_second.wait_recv()
        passed = self.region(self.second, 0)
        self.half_first = self.sender.start(passed, passed, {"cols": self.first})
        self.partner(self.region(self.second))

    def last_hop(self):
        self.half_second.wait_recv()
        self.partner(self.region(self.third, 1))
        self.half_first.wait_recv()
        self.partner(self.region(self.third, 0))

    def finish(self):
        for copy in self.pending:
            copy.wait_recv()


def meet(along_rows, in_slab):
    barrier = pltpu.get_barrier_semaphore()
    devices = []
    if along_rows:
        row = lax.axis_index("rows")
        count = lax.axis_size("rows")
        devices += [{"rows": lax.rem(row + 1, count)}, {"rows": lax.rem(row + count - 1, count)}]
    if in_slab:
        col = lax.axis_index("cols")
        devices += [{"cols": col + 1 - 2 * lax.rem(col, 2)}, {"cols": lax.rem(col + 2, 4)}]
        devices += [{"space": 1 - lax.axis_index("space")}]
    for device in devices:
        pl.semaphore_signal(barrier, inc=1, device_id=device, device_id_type=pl.DeviceIdType.MESH)
    pl.semaphore_wait(barrier, len(devices))


def send_panels(sender, piece_ref, window_ref):
    row = lax.axis_index("rows")
    count = lax.axis_size("rows")
    height, slab = piece_ref.shape
    own = height // 3
    above = sender.start(
        piece_ref.at[pl.ds(own, 2 * own), :],
        window_ref.at[pl.ds(0, 2 * own), pl.ds(0, slab)],
        {"rows": lax.rem(row + 1, count)},
    )
    below = sender.start(
        piece_ref.at[pl.ds(0, 2 * own), :],
        window_ref.at[pl.ds(own, 2 * own), pl.ds(2 * slab, slab)],
        {"rows": lax.rem(row + count - 1, count)},
    )
    return above, below


def fill_rest(piece_ref, window_ref, slab, own):
    zero = jnp.zeros((own, slab), jnp.float32)
    window_ref[2 * own :, :slab] = zero
    window_ref[:own, 2 * slab :] = zero


def exchange_kernel(piece_ref, window_ref, send_sems, recv_sems):
    meet(True, False)
    sender = Sender(send_sems, recv_sems)
    copies = send_panels(sender, piece_ref, window_ref)
    height, slab = piece_ref.shape
    window_ref[:, slab : 2 * slab] = piece_ref[...]
    fill_rest(piece_ref, window_ref, slab, height // 3)
    for copy in copies:
        copy.wait_recv()
    sender.finish()


def gather_kernel(block_ref, out_ref, send_sems, recv_sems):
    meet(False, True)
    sender = Sender(send_sems, recv_sems)
    height, width = block_ref.shape
    gather = Gather(sender, block_ref, out_ref, (0, height), (0, width))
    out_ref[lax.axis_index(GROUP)] = block_ref[...]
    gather.relay()
    gather.last_hop()
    gather.finish()
    sender.finish()


def both_kernel(piece_ref, block_ref, window_ref, out_ref, send_sems, recv_sems):
    meet(True, True)
    sender = Sender(send_sems, recv_sems)
    copies = send_panels(sender, piece_ref, window_ref)
    height, width = block_ref.shape
    gather = Gather(sender, block_ref, out_ref, (0, height), (0, width))
    out_ref[lax.axis_index(GROUP)] = block_ref[...]
    height, slab = piece_ref.shape
    window_ref[:, slab : 2 * slab] = piece_ref[...]
    fill_rest(piece_ref, window_ref, slab, height // 3)
    gather.relay()
    gather.last_hop()
    gather.finish()
    for copy in copies:
        copy.wait_recv()
    sender.finish()


def window_kernel(piece_ref, out_ref, send_sems, recv_sems):
    meet(True, True)
    sender = Sender(send_sems, recv_sems)
    height, slab = piece_ref.shape
    own = height // 3
    home = lax.axis_index(GROUP)
    above, below = send_panels(sender, piece_ref, out_ref.at[home])
    gathers = [Gather(sender, piece_ref, out_ref, (0, height), (slab, slab))]
    out_ref[home, :, slab : 2 * slab] = piece_ref[...]
    zero = jnp.zeros((own, slab), jnp.float32)
    for owner in range(out_ref.shape[0]):
        out_ref[owner, 2 * own :, :slab] = zero
        out_ref[owner, :own, 2 * slab :] = zero
    for copy, start, lane in ((above, 0, 0), (below, own, 2 * slab)):
        copy.wait_recv()
        source = out_ref.at[home, pl.ds(start, 2 * own), pl.ds(lane, slab)]
        gathers.append(Gather(sender, source, out_ref, (start, 2 * own), (lane, slab)))
    for gather in gathers:
        gather.relay()
    for gather in gathers:
        gather.last_hop()
    for gather in gathers:
        gather.finish()
    sender.finish()


def exchange_call(kernel, copies, collective, shapes, *operands):
    space = pl.BlockSpec(memory_space=pltpu.VMEM)
    return pl.pallas_call(
        kernel,
        out_shape=[jax.ShapeDtypeStruct(shape, jnp.float32) for shape in shapes],
        in_specs=[space] * len(operands),
        out_specs=[space] * len(shapes),
        scratch_shapes=[pltpu.SemaphoreType.DMA((copies,)), pltpu.SemaphoreType.DMA((copies,))],
        compiler_params=pltpu.CompilerParams(
            collective_id=collective, has_side_effects=True, vmem_limit_bytes=40 * 2**20
        ),
    )(*operands)


def split(value):
    upper = value.astype(jnp.bfloat16)
    return upper, (value - upper.astype(jnp.float32)).astype(jnp.bfloat16)


def dot_f32(leftside, rightside):
    return jnp.dot(leftside, rightside, preferred_element_type=jnp.float32)


def dot_split(leftside, rightside):
    left_hi, left_lo = leftside
    right_hi, right_lo = rightside
    return (
        dot_f32(left_hi, right_hi)
        + dot_f32(left_hi, right_lo)
        + dot_f32(left_lo, right_hi)
    )


def submatrix_kernel(maxb, slab_blocks, pos_ref, count_ref, offs_ref, gathered_ref, out_ref, rows_ref):
    width = gathered_ref.shape[1] // 3
    slab = gathered_ref.shape[2] // 3
    per_piece = width // BLK
    index = pl.program_id(0)
    live = count_ref[index]

    def place(p, carry):
        block = pos_ref[index, p]
        panel = block // slab_blocks
        within = lax.rem(block, slab_blocks)
        owner = within // per_piece
        start = pl.multiple_of(panel * width + lax.rem(within, per_piece) * BLK, BLK)
        target = pl.multiple_of(p * BLK, BLK)
        values = gathered_ref[owner, pl.ds(start, BLK), :]
        rows_ref[pl.ds(target, BLK), :] = jnp.where(p < live, values, 0.0)
        return carry

    lax.fori_loop(0, maxb, place, 0)
    offsets = offs_ref[0]
    order = maxb * BLK
    select = lax.broadcasted_iota(jnp.int32, (3 * slab, order), 0) == offsets
    select = jnp.where(select, 1.0, 0.0).astype(jnp.bfloat16)
    rows_hi, rows_lo = split(rows_ref[...])
    assembled = dot_f32(rows_hi, select) + dot_f32(rows_lo, select)
    columns = lax.broadcasted_iota(jnp.int32, (order, order), 1)
    assembled = jnp.where(columns < live * BLK, assembled, 0.0)
    symmetric = 0.5 * (assembled + assembled.T)
    total = jnp.sum(jnp.sum(symmetric * symmetric, axis=1, keepdims=True), axis=0, keepdims=True)
    live_order = jnp.full((1, 1), live * BLK, jnp.int32).astype(jnp.float32)
    iterate = symmetric * (jnp.sqrt(live_order) / (2.0 * jnp.sqrt(total + 1e-06)))
    parts = split(iterate)
    square = split(dot_split(parts, parts))
    iterate = 1.5 * iterate - 0.5 * dot_split(parts, square)
    home = iterate[:BLK]
    parts = split(iterate)
    once = dot_split((parts[0][:BLK], parts[1][:BLK]), parts)
    home = 1.5 * home - 0.5 * dot_split(split(once), parts)
    row = lax.broadcasted_iota(jnp.int32, (BLK, order), 0)
    column = lax.broadcasted_iota(jnp.int32, (BLK, order), 1)
    density = 0.5 * (jnp.where(row == column, 1.0, 0.0) - home)
    density_hi, density_lo = split(density)
    spread = functools.partial(
        lax.dot_general,
        dimension_numbers=(((1,), (1,)), ((), ())),
        preferred_element_type=jnp.float32,
    )
    out_ref[...] = spread(density_hi, select) + spread(density_lo, select)


def submatrices(gathered, sub_blocks, sub_count):
    own_blocks, maxb = sub_blocks.shape
    slab = gathered.shape[2] // 3
    order = maxb * BLK
    offsets = sub_blocks[:, :, None] * BLK + jnp.arange(BLK, dtype=jnp.int32)
    offsets = offsets.reshape(own_blocks, 1, order)
    return pl.pallas_call(
        functools.partial(submatrix_kernel, maxb, slab // BLK),
        out_shape=jax.ShapeDtypeStruct((own_blocks * BLK, 3 * slab), jnp.float32),
        grid_spec=pltpu.PrefetchScalarGridSpec(
            num_scalar_prefetch=2,
            grid=(own_blocks,),
            in_specs=[
                pl.BlockSpec((1, 1, order), lambda i, *_: (i, 0, 0)),
                pl.BlockSpec(memory_space=pltpu.VMEM),
            ],
            out_specs=pl.BlockSpec((BLK, 3 * slab), lambda i, *_: (i, 0)),
            scratch_shapes=[pltpu.VMEM((order, 3 * slab), jnp.float32)],
        ),
    )(sub_blocks, sub_count, offsets, gathered)


def shards(hamiltonian, correlation_root, pattern, sub_blocks, sub_count):
    slab = correlation_root.shape[0]
    slab_blocks = slab // BLK
    own = hamiltonian.shape[0]
    parts = slab // own
    slab_index = lax.axis_index("rows")
    home = lax.axis_index(GROUP)
    slab_pattern = lax.dynamic_slice_in_dim(pattern, slab_index * slab_blocks, slab_blocks, 0)
    weights = slab_pattern.astype(jnp.float32)
    own_pattern = lax.dynamic_slice_in_dim(weights, home * (own // BLK), own // BLK, 0)
    own_mask = jnp.repeat(jnp.repeat(own_pattern, BLK, axis=0), BLK, axis=1)
    piece_pattern = lax.dynamic_index_in_dim(
        weights.reshape(slab_blocks, 3, parts, own // BLK), home, 2, keepdims=False
    )
    piece_mask = jnp.repeat(jnp.repeat(piece_pattern.transpose(1, 2, 0), BLK, axis=1), BLK, axis=2)
    piece_mask = piece_mask.reshape(3 * own, slab)

    root_piece = lax.dynamic_index_in_dim(
        correlation_root.reshape(slab, 3, parts, own), home, 2, keepdims=False
    ).transpose(1, 2, 0).reshape(3 * own, slab)
    window_shape = (3 * own, 3 * slab)
    block_shape = (parts, own, 3 * slab)
    root_window, whole_hamiltonian = exchange_call(
        both_kernel, 11, 1, [window_shape, block_shape], root_piece, hamiltonian
    )

    def step(left, window):
        return piece_mask * multiply_nt(window, left.reshape(slab, 3 * slab))

    half_done = step(whole_hamiltonian, root_window)
    (done_window,) = exchange_call(exchange_kernel, 2, 2, [window_shape], half_done)
    ortho = step(correlation_root, done_window)
    (gathered,) = exchange_call(window_kernel, 29, 3, [(parts, *window_shape)], ortho)
    home_density = submatrices(gathered, sub_blocks, sub_count)
    (whole_density,) = exchange_call(gather_kernel, 9, 4, [block_shape], home_density)
    half_back = step(whole_density, root_window)
    (back_window,) = exchange_call(exchange_kernel, 2, 5, [window_shape], half_back)
    density = multiply_nt(back_window, correlation_root).reshape(3, own, parts, own)
    density = lax.all_to_all(density.transpose(2, 3, 0, 1), GROUP, 0, 0, tiled=False)
    density = own_mask * density.transpose(1, 2, 0, 3).reshape(own, 3 * slab)
    return density, jnp.sum(density, axis=1)


def solution(mesh):
    return jax.shard_map(
        shards,
        mesh=mesh,
        in_specs=(
            P(("rows", "cols", "space"), None),
            P("rows", None),
            P(),
            P(("rows", "cols", "space"), None),
            P(("rows", "cols", "space")),
        ),
        out_specs=(P(("rows", "cols", "space"), None), P(("rows", "cols", "space"))),
        check_vma=False,
    )
```
